32 devices in a mesh: groups: 2 (over y), branch: 4 (over z), leaf: 4 (over x, core).
Axes of the slice: x: 2, y: 2, z: 4, core: 2. Of those that a mesh axis runs over, the one named last changes fastest.
Arguments:
- queries: float32 [4096, 1024], P(('groups', 'branch', 'leaf')), parts along dimension 0, may hold values from -32 to 32
- leaf_keys: float32 [4096, 128], P(('groups', 'branch', 'leaf')), parts along dimension 0, may hold values from -6 to 6
- leaf_values: float32 [4096, 128], P(('groups', 'branch', 'leaf')), parts along dimension 0, may hold values from -6 to 6
- root_keys: float32 [512, 128], P(('groups', 'branch', 'leaf')), parts along dimension 0, may hold values from -12 to 12
- root_values: float32 [512, 128], P(('groups', 'branch', 'leaf')), parts along dimension 0, may hold values from -6 to 6
- branch_keys: float32 [2048, 128], P(('groups', 'branch', 'leaf')), parts along dimension 0, may hold values from -6 to 6
- branch_values: float32 [2048, 128], P(('groups', 'branch', 'leaf')), parts along dimension 0, may hold values from -6 to 6
- d_out: float32 [4096, 1024], P(('groups', 'branch', 'leaf')), parts along dimension 0, may hold values from -6 to 6
- leaf_len: int32 [32], P(('groups', 'branch', 'leaf')), parts along dimension 0, may hold values from 1 to 128, 1280 in all
- leaf_parent: int32 [32], P(('groups', 'branch', 'leaf')), parts along dimension 0, may hold values from 0 to 255
- root_cut: int32 [8], P(('groups', 'branch')), parts along dimension 0, may hold values from 128 to 256
Outputs:
- attended: float32 [4096, 1024], P(('groups', 'branch', 'leaf')), parts along dimension 0
- d_queries: float32 [4096, 1024], P(('groups', 'branch', 'leaf')), parts along dimension 0
- d_root_kv: float32 [512, 256], P(('groups', 'branch', 'leaf')), parts along dimension 0
- d_branch_kv: float32 [2048, 256], P(('groups', 'branch', 'leaf')), parts along dimension 0
- d_leaf_kv: float32 [4096, 256], P(('groups', 'branch', 'leaf')), parts along dimension 0
The draws below stay inside these ranges and needn't reach their ends.
There are 2 independent parts, one for each index of `groups`. The reference program is written for one: setup_inputs(seed, part) draws one part's arguments, and reference() takes and returns one part's arrays. A program takes and returns all parts, laid end to end along the dimension named above; each array names one. Nothing has to cross between parts.
Inputs may be any that keep to these rules, and one draw needn't show every extreme that they name: `leaf_len`: the lengths of one tree sum to 1280, and some leaf holds 128 live tokens.
All inputs are finite; a program needn't handle non-finite values. No bound on the sum of `leaf_len` on one device may be relied on, other than what follows from the above.
Results may differ from the reference program's by a relative error of at most 0.0003.
Values sent between devices are 32-bit elements; how exact they have to be, the bound alone decides.
A program may use at most 64 MiB of HBM per device.

```python
import math
import jax
import jax.numpy as jnp
import numpy as np
from jax import lax

HEAD_DIM = 128
HEADS = 8
LEAF_CAP = 128
ROOT = 256
BRANCH = 256
BRANCH_ALL = 1024
LEAVES = 16
LEAF_TOTAL = 2048
N_BRANCH = 4
N_LEAF = 4


def draw_root_keys(key, part):
    noise_key = jax.random.fold_in(jax.random.fold_in(key, 11), 0)
    entries = jnp.clip(jax.random.normal(noise_key, (ROOT, HEAD_DIM), jnp.float32), -4.0, 4.0)
    return entries.astype(jnp.float32)


def draw_queries(key, part):
    noise_key = jax.random.fold_in(jax.random.fold_in(key, 23), 0)
    entries = 2.5 * jnp.clip(jax.random.normal(noise_key, (LEAF_TOTAL, HEADS, HEAD_DIM), jnp.float32), -4.0, 4.0)
    return entries.reshape(LEAF_TOTAL, HEADS * HEAD_DIM).astype(jnp.float32)


def touch_ends(drawn, own_key, low, top_value):
    longest = drawn.shape.index(max(drawn.shape))
    spots = []
    for shift in (0, 1):
        where = [jax.random.randint(jax.random.fold_in(own_key, axis), (), 0, length) for axis, length in enumerate(drawn.shape)]
        where[longest] = (where[longest] + shift) % drawn.shape[longest]
        spots.append(tuple(where))
    return drawn.at[spots[0]].set(low).at[spots[1]].set(top_value)


def level_of(stream_key, dims, cuts, low, high):
    level = 1.0
    for position, parts in cuts:
        heights = jax.random.uniform(jax.random.fold_in(jax.random.fold_in(stream_key, 6), position), (parts,), jnp.float32, low / len(cuts), high / len(cuts))
        level = level * jnp.repeat(jnp.exp(heights), dims[position] // parts).reshape((-1,) + (1,) * (len(dims) - 1 - position))
    return level


def profile(number_of, total, reach, skew):
    weights = [(1 << 20) // math.isqrt(standing ** skew) + 1 for standing in range(2, number_of + 1)]
    surplus, counts = total - reach - (number_of - 1), [1] * (number_of - 1)
    while surplus > 0:
        free = [i for i in range(number_of - 1) if counts[i] < reach]
        whole, left = sum([weights[i] for i in free]), surplus
        for i in free:
            more = min(reach - counts[i], max(1, left * weights[i] // whole), surplus)
            counts[i] = counts[i] + more
            surplus = surplus - more
    return np.array([reach] + counts)


def uneven_parts(own_key, number_of, total, limit, lean):
    if number_of == 2:
        one = jax.random.randint(own_key, (), max(1, total - limit), min(limit, total - 1) + 1)
        return jnp.stack([one, total - one])
    sizes = jnp.asarray(profile(number_of, total, limit, lean), jnp.int32)
    pairs = (number_of - 1) // 2
    giver, sink = sizes[1:1 + 2 * pairs:2], sizes[2:2 + 2 * pairs:2]
    margin = jnp.minimum(giver - 1, limit - sink)
    shifted = jax.random.randint(jax.random.fold_in(own_key, 1), (pairs,), 0, 1 << 20) % (margin + 1)
    sizes = sizes.at[1:1 + 2 * pairs:2].set(giver - shifted).at[2:2 + 2 * pairs:2].set(sink + shifted)
    return sizes[jax.random.permutation(jax.random.fold_in(own_key, 2), number_of)]


def normal_values(key, extent, scale, limit, cuts=(), kind=jnp.bfloat16):
    gain = level_of(key, extent, cuts, -0.22, 0.18) if cuts else 1.0
    values = jax.random.normal(key, extent, jnp.float32) * scale * gain
    return jnp.minimum(jnp.maximum(values, -limit), limit).astype(kind)


def setup_inputs(seed: int = 0, part: int = 0) -> dict:
    key_list = jax.random.split(jax.random.key(seed), 12)
    part_splits = jax.random.split(jax.random.fold_in(key_list[11], part), 12)
    return {
        "queries": draw_queries(jax.random.fold_in(jax.random.fold_in(key_list[11], part), 71), part),
        "leaf_keys": normal_values(part_splits[1], (LEAF_TOTAL, HEAD_DIM), 1.5, 6.0, ((0, 16),), jnp.float32),
        "leaf_values": normal_values(part_splits[2], (LEAF_TOTAL, HEAD_DIM), 1.0, 6.0, ((0, 16),), jnp.float32),
        "root_keys": draw_root_keys(jax.random.fold_in(jax.random.fold_in(key_list[11], part), 71), part),
        "root_values": normal_values(part_splits[4], (ROOT, HEAD_DIM), 1.0, 6.0, ((0, 16),), jnp.float32),
        "branch_keys": normal_values(part_splits[5], (BRANCH_ALL, HEAD_DIM), 1.0, 6.0, ((0, 16),), jnp.float32),
        "branch_values": normal_values(part_splits[6], (BRANCH_ALL, HEAD_DIM), 1.0, 6.0, ((0, 16),), jnp.float32),
        "d_out": normal_values(part_splits[7], (LEAF_TOTAL, HEADS * HEAD_DIM), 1.0, 6.0, ((0, 16),), jnp.float32),
        "leaf_len": uneven_parts(part_splits[8], LEAVES, LEAVES * (5 * LEAF_CAP // 8), LEAF_CAP, 2).astype(jnp.int32),
        "leaf_parent": touch_ends(jax.random.randint(part_splits[9], (LEAVES,), 0, BRANCH), jax.random.fold_in(part_splits[9], 1), 0, BRANCH - 1).astype(jnp.int32),
        "root_cut": touch_ends(jax.random.randint(part_splits[10], (N_BRANCH,), ROOT // 2, ROOT + 1), jax.random.fold_in(part_splits[10], 1), ROOT // 2, ROOT).astype(jnp.int32),
    }


def leaf_attention(query_heads, whole_root_keys, whole_root_values, slice_keys, slice_values, own_keys, own_values, root_limit, parent, length):
    head_dim = own_keys.shape[1]
    score_scale = 1.0 / math.sqrt(head_dim)
    highest = lax.Precision.HIGHEST
    all_keys = jnp.concatenate([whole_root_keys, slice_keys, own_keys], axis=0)
    all_values = jnp.concatenate([whole_root_values, slice_values, own_values], axis=0)
    columns = jnp.arange(all_keys.shape[0], dtype=jnp.int32)[None, :]
    positions = jnp.arange(own_keys.shape[0], dtype=jnp.int32)[:, None]
    in_root = columns < root_limit
    in_slice = (columns >= ROOT) & (columns < ROOT + BRANCH) & (columns - ROOT <= parent)
    in_leaf = (columns >= ROOT + BRANCH) & (columns - ROOT - BRANCH <= positions)
    visible = in_root | in_slice | in_leaf
    scores = jnp.einsum('thd,kd->thk', query_heads, all_keys, precision=highest) * score_scale
    scores = jnp.where(visible[:, None, :], scores, -jnp.inf)
    row_max = lax.stop_gradient(lax.optimization_barrier(jnp.max(scores, axis=-1, keepdims=True)))
    raised = jnp.exp(scores - row_max)
    weights = raised / lax.optimization_barrier(jnp.sum(raised, axis=-1, keepdims=True))
    mixture = jnp.einsum('thk,kd->thd', weights, all_values, precision=highest)
    live_rows = (positions[:, 0] < length).astype(jnp.float32)
    return mixture * live_rows[:, None, None]

def reference(queries, leaf_keys, leaf_values, root_keys, root_values, branch_keys, branch_values, d_out, leaf_len, leaf_parent, root_cut):
    query_all = queries.reshape(LEAVES, LEAF_CAP, HEADS, HEAD_DIM)
    cotangent_all = d_out.reshape(LEAVES, LEAF_CAP, HEADS, HEAD_DIM)
    own_keys_all = leaf_keys.reshape(LEAVES, LEAF_CAP, HEAD_DIM)
    own_values_all = leaf_values.reshape(LEAVES, LEAF_CAP, HEAD_DIM)

    def per_leaf(running, inputs):
        root_total, slice_total = running
        leaf_index, query_heads, own_keys, own_values, cotangent, length, parent = inputs
        slice_index = (leaf_index // N_LEAF).astype(jnp.int32)
        offset = (slice_index * BRANCH).astype(jnp.int32)
        slice_keys = lax.dynamic_slice_in_dim(branch_keys, offset, BRANCH, 0)
        slice_values = lax.dynamic_slice_in_dim(branch_values, offset, BRANCH, 0)
        root_limit = lax.dynamic_index_in_dim(root_cut, slice_index, keepdims=False)

        def forward(query_in, rootk_in, rootv_in, slicek_in, slicev_in, ownk_in, ownv_in):
            return leaf_attention(query_in, rootk_in, rootv_in, slicek_in, slicev_in, ownk_in, ownv_in, root_limit, parent, length)
        mixture, pullback = jax.vjp(forward, query_heads, root_keys, root_values, slice_keys, slice_values, own_keys, own_values)
        gradients = pullback(cotangent)
        root_total = root_total + jnp.concatenate([gradients[1], gradients[2]], axis=1)
        slice_piece = jnp.concatenate([gradients[3], gradients[4]], axis=1)
        current = lax.dynamic_slice_in_dim(slice_total, offset, BRANCH, 0)
        slice_total = lax.dynamic_update_slice_in_dim(slice_total, current + slice_piece, offset, 0)
        outputs = (mixture.reshape(LEAF_CAP, HEADS * HEAD_DIM), gradients[0].reshape(LEAF_CAP, HEADS * HEAD_DIM), jnp.concatenate([gradients[5], gradients[6]], axis=1))
        return ((root_total, slice_total), outputs)
    initial = (jnp.zeros((ROOT, 2 * HEAD_DIM), jnp.float32), jnp.zeros((BRANCH_ALL, 2 * HEAD_DIM), jnp.float32))
    leaf_ids = jnp.arange(LEAVES, dtype=jnp.int32)
    finals, stacked = lax.scan(per_leaf, initial, (leaf_ids, query_all, own_keys_all, own_values_all, cotangent_all, leaf_len, leaf_parent))
    root_total, slice_total = finals
    attended, d_queries, d_leaf = stacked
    return (attended.reshape(LEAF_TOTAL, HEADS * HEAD_DIM), d_queries.reshape(LEAF_TOTAL, HEADS * HEAD_DIM), root_total, slice_total, d_leaf.reshape(LEAF_TOTAL, 2 * HEAD_DIM))
```

```python
import functools
import math

import jax
import jax.numpy as jnp
from jax import lax
from jax.experimental import pallas as pl
from jax.experimental.pallas import tpu as pltpu
from jax.sharding import PartitionSpec as P

f32 = jnp.float32
bf16 = jnp.bfloat16
hidden = -1e30


def split2(x):
    high = x.astype(bf16)
    return high, (x - high.astype(f32)).astype(bf16)


def split3(x):
    high = x.astype(bf16)
    rest = x - high.astype(f32)
    middle = rest.astype(bf16)
    return high, middle, (rest - middle.astype(f32)).astype(bf16)


def mm(a, b):
    return lax.dot_general(a, b, (((1,), (0,)), ((), ())), preferred_element_type=f32)


def mmt(a, b):
    return lax.dot_general(a, b, (((1,), (1,)), ((), ())), preferred_element_type=f32)


def side(*parts):
    return jnp.concatenate(parts, axis=1)


def kernel(
    nb, nx, nc, dims,
    q_hbm, lk_hbm, lv_hbm, rk_hbm, rv_hbm, bk_hbm, bv_hbm, do_hbm, len_ref, par_ref, cut_ref,
    att_hbm, dq_hbm, droot_ref, dslice_ref, dleaf_ref,
    q_ref, do_ref, leaf_ref, rootb, sliceb,
    qs, cs, ks, vs, kt, vt, sc, dp, dkv,
    att_ref, dqv_ref,
    rc_root, rc_slice, sn_root, sn_slice, rv_root, rv_slice,
    ld_sem, st_sem, gs_root, gr_root, gs_slice, gr_slice, cs_sem, cr_sem,
    ss_root, sr_root, ss_slice, sr_slice, es_sem, er_sem,
):
    T, H, D, r_rows, b_rows = dims
    R = T * H
    n_root = nb * nx * nc * r_rows
    n_slice = nx * nc * b_rows
    n_keys = n_root + n_slice + T
    scale = 1.0 / math.sqrt(D)
    g = lax.axis_index("groups")
    b = lax.axis_index("branch")
    leaf = lax.axis_index("leaf")
    x = leaf // nc
    c = leaf % nc
    pair = 2 * T if H % 2 == 0 else T
    per = pair // T
    n_pair = R // pair

    def dev(bb, xx, cc):
        return (g, bb, xx * nc + cc)

    def shifted(sb, sx):
        return lax.rem(b + sb, nb), lax.rem(x + sx, nx)

    peers = [(sb, sx) for sb in range(nb) for sx in range(nx) if sb or sx]
    other = lax.rem(c + 1, nc)

    loads = [
        (rk_hbm, rootb.at[b, x, c, 0]),
        (rv_hbm, rootb.at[b, x, c, 1]),
        (bk_hbm, sliceb.at[x, c, 0]),
        (bv_hbm, sliceb.at[x, c, 1]),
        (lk_hbm, leaf_ref.at[0]),
        (lv_hbm, leaf_ref.at[1]),
        (q_hbm, q_ref),
        (do_hbm, do_ref),
    ]
    loads = [pltpu.make_async_copy(s, d, ld_sem.at[i]) for i, (s, d) in enumerate(loads)]
    for cp in loads:
        cp.start()

    barrier = pltpu.get_barrier_semaphore()
    for sb, sx in peers:
        bb, xx = shifted(sb, sx)
        pl.semaphore_signal(barrier, inc=1, device_id=dev(bb, xx, c), device_id_type=pl.DeviceIdType.MESH)
    if nc == 2:
        pl.semaphore_signal(barrier, inc=1, device_id=dev(b, x, other), device_id_type=pl.DeviceIdType.MESH)
    pl.semaphore_wait(barrier, len(peers) + (nc == 2))

    def remote(src, dst, s_sem, r_sem, where):
        return pltpu.make_async_remote_copy(
            src_ref=src, dst_ref=dst, send_sem=s_sem, recv_sem=r_sem,
            device_id=where, device_id_type=pl.DeviceIdType.MESH,
        )

    for cp in loads[:4]:
        cp.wait()
    slice_sends, root_sends = [], []
    for sx in range(1, nx):
        bb, xx = shifted(0, sx)
        blk = sliceb.at[x, c]
        slice_sends.append(remote(blk, blk, gs_slice.at[sx], gr_slice.at[sx], dev(b, xx, c)))
    for i, (sb, sx) in enumerate(peers):
        bb, xx = shifted(sb, sx)
        blk = rootb.at[b, x, c]
        root_sends.append(remote(blk, blk, gs_root.at[i], gr_root.at[i], dev(bb, xx, c)))
    for cp in root_sends + slice_sends:
        cp.start()

    for cp in loads[4:]:
        cp.wait()
    live = lax.broadcasted_iota(jnp.int32, (T, D), 0) < len_ref[0]
    for h in range(H):
        cols = slice(h * D, (h + 1) * D)
        rows = slice(h * T, (h + 1) * T)
        q1, q2, q3 = split3(q_ref[:, cols])
        qs[0, rows], qs[1, rows], qs[2, rows] = q1, q2, q3
        c1, c2 = split2(jnp.where(live, do_ref[:, cols], 0.0))
        cs[0, rows], cs[1, rows] = c1, c2

    def stage(first, keys, values):
        count = keys.shape[0]
        span = slice(first, first + count)
        k1, k2, k3 = split3(keys)
        ks[span, :] = side(k1, k2, k3)
        v1, v2 = split2(values)
        vs[span, :] = side(v1, v2)
        ka, kb = split2(keys.T)
        kt[:D, span] = ka
        kt[D:, span] = kb
        va, vb = split2(values.T)
        vt[:D, span] = va
        vt[D:, span] = vb

    def score(first, count, seen):
        step = min(count, 256)

        def body(p, carry):
            rows = pl.ds(pl.multiple_of(p * pair, pair), pair)
            q1, q2, q3 = qs[0, rows, :], qs[1, rows, :], qs[2, rows, :]
            c1, c2 = cs[0, rows, :], cs[1, rows, :]
            qa, qb, qc = side(q1, q1), side(q2, q2), side(q3, q1)
            ca, cb = side(c1, c1), side(c2, c2)
            for lo in range(0, count, step):
                span = slice(first + lo, first + lo + step)
                k12 = ks[span, : 2 * D]
                k13 = side(ks[span, :D], ks[span, 2 * D :])
                s = mmt(k12, qa) + (mmt(k12, qb) + mmt(k13, qc))
                sc[span, rows] = jnp.where(seen(lo, step), s * scale, hidden)
                v12 = vs[span, :]
                dp[span, rows] = mmt(v12, ca) + mmt(v12, cb)
            return carry

        lax.fori_loop(0, n_pair, body, 0)

    def index_of(lo, step):
        return lo + lax.broadcasted_iota(jnp.int32, (step, pair), 0)

    def slot_of(step):
        return lax.broadcasted_iota(jnp.int32, (step, pair), 1) % T

    stage(n_root + n_slice, leaf_ref[0], leaf_ref[1])
    score(n_root + n_slice, T, lambda lo, step: index_of(lo, step) <= slot_of(step))

    core_sends = []
    for sx in range(1, nx):
        blk = sliceb.at[lax.rem(x + nx - sx, nx), c]
        remote(blk, blk, gs_slice.at[sx], gr_slice.at[sx], dev(b, x, c)).wait_recv()
    if nc == 2:
        cp = remote(sliceb.at[:, c], sliceb.at[:, c], cs_sem.at[0], cr_sem.at[0], dev(b, x, other))
        cp.start()
        core_sends.append(cp)
    for i, (sb, sx) in enumerate(peers):
        blk = rootb.at[lax.rem(b + nb - sb, nb), lax.rem(x + nx - sx, nx), c]
        remote(blk, blk, gs_root.at[i], gr_root.at[i], dev(b, x, c)).wait_recv()
    if nc == 2:
        cp = remote(rootb.at[:, :, c], rootb.at[:, :, c], cs_sem.at[1], cr_sem.at[1], dev(b, x, other))
        cp.start()
        core_sends.append(cp)
        remote(sliceb.at[:, other], sliceb.at[:, other], cs_sem.at[0], cr_sem.at[0], dev(b, x, other)).wait_recv()
    stage(
        n_root,
        sliceb[:, :, 0].reshape(n_slice, D),
        sliceb[:, :, 1].reshape(n_slice, D),
    )
    score(n_root, n_slice, lambda lo, step: index_of(lo, step) <= par_ref[0])
    if nc == 2:
        remote(rootb.at[:, :, other], rootb.at[:, :, other], cs_sem.at[1], cr_sem.at[1], dev(b, x, other)).wait_recv()
    stage(
        0,
        rootb[:, :, :, 0].reshape(n_root, D),
        rootb[:, :, :, 1].reshape(n_root, D),
    )
    score(0, n_root, lambda lo, step: index_of(lo, step) < cut_ref[0])

    chunk = 128

    def soften(p, carry):
        rows = pl.ds(pl.multiple_of(p * pair, pair), pair)
        spans = [slice(lo, lo + chunk) for lo in range(0, n_keys, chunk)]
        top = None
        for span in spans:
            m = jnp.max(sc[span, rows], axis=0, keepdims=True)
            top = m if top is None else jnp.maximum(top, m)
        total = jnp.zeros((1, pair), f32)
        dot = jnp.zeros((1, pair), f32)
        for span in spans:
            e = jnp.exp(sc[span, rows] - top)
            sc[span, rows] = e
            total = total + jnp.sum(e, axis=0, keepdims=True)
            dot = dot + jnp.sum(e * dp[span, rows], axis=0, keepdims=True)
        inverse = 1.0 / total
        dot = dot * inverse
        for span in spans:
            w = sc[span, rows] * inverse
            sc[span, rows] = w
            dp[span, rows] = w * (dp[span, rows] - dot) * scale
        return carry

    lax.fori_loop(0, n_pair, soften, 0)

    def key_gradients(first, step):
        span = pl.ds(first, step)
        s1, s2 = split2(dp[span, :])
        q12 = side(qs[0], qs[1])
        a = mm(s1, q12) + mm(s2, q12)
        w1, w2 = split2(sc[span, :])
        c12 = side(cs[0], cs[1])
        v = mm(w1, c12) + mm(w2, c12)
        return side(a[:, :D] + a[:, D:], v[:, :D] + v[:, D:])

    def gradient_block(i, carry):
        at = pl.multiple_of(i * chunk, chunk)
        dkv[pl.ds(at, chunk), :] = key_gradients(at, chunk)
        return carry

    root_g = dkv.at[:n_root].reshape(nb, nx, nc, r_rows, 2 * D)
    slice_g = dkv.at[n_root : n_root + n_slice].reshape(nx, nc, b_rows, 2 * D)
    lax.fori_loop(0, n_root // chunk, gradient_block, 0)
    ex = []
    if nc == 2:
        cp = remote(root_g.at[:, :, other], rc_root, es_sem.at[0], er_sem.at[0], dev(b, x, other))
        cp.start()
        ex.append(cp)
    lax.fori_loop(n_root // chunk, (n_root + n_slice) // chunk, gradient_block, 0)
    if nc == 2:
        cp = remote(slice_g.at[:, other], rc_slice, es_sem.at[1], er_sem.at[1], dev(b, x, other))
        cp.start()
        ex.append(cp)
        ex[0].wait_recv()
    mine = root_g[:, :, c]
    sn_root[...] = mine + rc_root[...] if nc == 2 else mine
    fin_root = []
    for i, (sb, sx) in enumerate(peers):
        bb, xx = shifted(sb, sx)
        fin_root.append(remote(sn_root.at[bb, xx], rv_root.at[i], ss_root.at[i], sr_root.at[i], dev(bb, xx, c)))
        fin_root[-1].start()
    if nc == 2:
        ex[1].wait_recv()
    mine = slice_g[:, c]
    sn_slice[...] = mine + rc_slice[...] if nc == 2 else mine
    fin_slice = []
    for sx in range(1, nx):
        bb, xx = shifted(0, sx)
        fin_slice.append(
            remote(sn_slice.at[xx], rv_slice.at[sx - 1], ss_slice.at[sx], sr_slice.at[sx], dev(b, xx, c))
        )
        fin_slice[-1].start()

    def outputs(p, carry):
        rows = pl.ds(pl.multiple_of(p * pair, pair), pair)
        w1, w2 = split2(sc[:, rows])
        m = mm(vt[...], w1) + mm(vt[...], w2)
        m = m[:D] + m[D:]
        s1, s2 = split2(dp[:, rows])
        n = mm(kt[...], s1) + mm(kt[...], s2)
        n = n[:D] + n[D:]
        for k in range(per):
            cols = pl.ds(pl.multiple_of(p * (per * D) + k * D, D), D)
            part = slice(k * T, (k + 1) * T)
            att_ref[:, cols] = jnp.where(live, m[:, part].T, 0.0)
            dqv_ref[:, cols] = n[:, part].T
        return carry

    lax.fori_loop(0, n_pair, outputs, 0)
    out_a = pltpu.make_async_copy(att_ref, att_hbm, st_sem.at[0])
    out_q = pltpu.make_async_copy(dqv_ref, dq_hbm, st_sem.at[1])
    out_a.start()
    out_q.start()
    dleaf_ref[...] = key_gradients(n_root + n_slice, T)

    for cp in fin_slice:
        cp.wait_recv()
    total = sn_slice[x]
    for i in range(nx - 1):
        total = total + rv_slice[i]
    dslice_ref[...] = total
    for cp in fin_root:
        cp.wait_recv()
    total = sn_root[b, x]
    for i in range(len(peers)):
        total = total + rv_root[i]
    droot_ref[...] = total
    for cp in root_sends + slice_sends + core_sends + ex + fin_root + fin_slice:
        cp.wait_send()
    out_a.wait()
    out_q.wait()


def shards(mesh, *args):
    queries, leaf_keys, _, root_keys, _, branch_keys = args[:6]
    T, width = queries.shape
    D = leaf_keys.shape[1]
    H = width // D
    r_rows, b_rows = root_keys.shape[0], branch_keys.shape[0]
    nb, nl = mesh.shape["branch"], mesh.shape["leaf"]
    nc = 2 if nl % 2 == 0 else 1
    nx = nl // nc
    R = T * H
    n_root, n_slice = nb * nl * r_rows, nl * b_rows
    n_keys = n_root + n_slice + T
    any_space = pl.BlockSpec(memory_space=pl.ANY)
    smem = pl.BlockSpec(memory_space=pltpu.SMEM)
    vmem = pl.BlockSpec(memory_space=pltpu.VMEM)
    V = pltpu.VMEM
    dma = pltpu.SemaphoreType.DMA
    np_ = max(nb * nx - 1, 1)
    scratch = [
        V((T, width), f32), V((T, width), f32), V((2, T, D), f32),
        V((nb, nx, nc, 2, r_rows, D), f32), V((nx, nc, 2, b_rows, D), f32),
        V((3, R, D), bf16), V((2, R, D), bf16),
        V((n_keys, 3 * D), bf16), V((n_keys, 2 * D), bf16),
        V((2 * D, n_keys), bf16), V((2 * D, n_keys), bf16),
        V((n_keys, R), f32), V((n_keys, R), f32), V((n_root + n_slice, 2 * D), f32),
        V((T, width), f32), V((T, width), f32),
        V((nb, nx, r_rows, 2 * D), f32), V((nx, b_rows, 2 * D), f32),
        V((nb, nx, r_rows, 2 * D), f32), V((nx, b_rows, 2 * D), f32),
        V((np_, r_rows, 2 * D), f32), V((max(nx - 1, 1), b_rows, 2 * D), f32),
        dma((8,)), dma((2,)), dma((np_,)), dma((np_,)), dma((nx,)), dma((nx,)), dma((2,)), dma((2,)),
        dma((np_,)), dma((np_,)), dma((nx,)), dma((nx,)), dma((2,)), dma((2,)),
    ]
    shape = lambda *s: jax.ShapeDtypeStruct(s, f32)
    return pl.pallas_call(
        functools.partial(kernel, nb, nx, nc, (T, H, D, r_rows, b_rows)),
        out_shape=(
            shape(T, width), shape(T, width), shape(r_rows, 2 * D), shape(b_rows, 2 * D), shape(T, 2 * D),
        ),
        in_specs=[any_space] * 8 + [smem] * 3,
        out_specs=(any_space, any_space, vmem, vmem, vmem),
        scratch_shapes=scratch,
        compiler_params=pltpu.CompilerParams(
            collective_id=0, has_side_effects=True, vmem_limit_bytes=60 * 1024 * 1024
        ),
        name="tree",
    )(*args)


def solution(mesh):
    rows = P(("groups", "branch", "leaf"), None)
    flat = P(("groups", "branch", "leaf"))
    return jax.shard_map(
        functools.partial(shards, mesh),
        mesh=mesh,
        in_specs=(rows,) * 8 + (flat, flat, P(("groups", "branch"))),
        out_specs=(rows,) * 5,
        check_vma=False,
    )
```

```python
import functools
import math

import jax
import jax.numpy as jnp
from jax import lax
from jax.experimental import pallas as pl
from jax.experimental.pallas import tpu as pltpu
from jax.sharding import PartitionSpec as P

f32 = jnp.float32
bf16 = jnp.bfloat16
hidden = -1e30


def split2(x):
    high = x.astype(bf16)
    return high, (x - high.astype(f32)).astype(bf16)


def split3(x):
    high = x.astype(bf16)
    rest = x - high.astype(f32)
    middle = rest.astype(bf16)
    return high, middle, (rest - middle.astype(f32)).astype(bf16)


def mm(a, b):
    return lax.dot_general(a, b, (((1,), (0,)), ((), ())), preferred_element_type=f32)


def mmt(a, b):
    return lax.dot_general(a, b, (((1,), (1,)), ((), ())), preferred_element_type=f32)


def side(*parts):
    return jnp.concatenate(parts, axis=1)


def kernel(
    nb, nx, nc, dims,
    q_hbm, lk_hbm, lv_hbm, rk_hbm, rv_hbm, bk_hbm, bv_hbm, do_hbm, len_hbm, par_hbm, cut_hbm,
    att_ref, dqv_ref, droot_ref, dslice_ref, dleaf_ref,
    q_ref, do_ref, leaf_ref, rootb, sliceb,
    qs, cs, ks, vs, kt, vt, sc, dp, dkv,
    len_ref, par_ref, cut_ref,
    rc_root, rc_slice, sn_root, sn_slice, rv_root, rv_slice,
    ld_sem, gs_root, gr_root, gs_slice, gr_slice, cs_sem, cr_sem,
    ss_root, sr_root, ss_slice, sr_slice, es_sem, er_sem,
):
    T, H, D, r_rows, b_rows = dims
    R = T * H
    n_root = nb * nx * nc * r_rows
    n_slice = nx * nc * b_rows
    n_keys = n_root + n_slice + T
    scale = 1.0 / math.sqrt(D)
    g = lax.axis_index("groups")
    b = lax.axis_index("branch")
    leaf = lax.axis_index("leaf")
    x = leaf // nc
    c = leaf % nc
    pair = 2 * T if H % 2 == 0 else T
    per = pair // T
    n_pair = R // pair

    def dev(bb, xx, cc):
        return (g, bb, xx * nc + cc)

    def shifted(sb, sx):
        return lax.rem(b + sb, nb), lax.rem(x + sx, nx)

    peers = [(sb, sx) for sb in range(nb) for sx in range(nx) if sb or sx]
    other = lax.rem(c + 1, nc)

    loads = [
        (rk_hbm, rootb.at[b, x, c, 0]),
        (rv_hbm, rootb.at[b, x, c, 1]),
        (bk_hbm, sliceb.at[x, c, 0]),
        (bv_hbm, sliceb.at[x, c, 1]),
        (lk_hbm, leaf_ref.at[0]),
        (lv_hbm, leaf_ref.at[1]),
        (q_hbm, q_ref),
        (do_hbm, do_ref),
        (len_hbm, len_ref),
        (par_hbm, par_ref),
        (cut_hbm, cut_ref),
    ]
    loads = [pltpu.make_async_copy(s, d, ld_sem.at[i]) for i, (s, d) in enumerate(loads)]
    for cp in loads:
        cp.start()

    barrier = pltpu.get_barrier_semaphore()
    for sb, sx in peers:
        bb, xx = shifted(sb, sx)
        pl.semaphore_signal(barrier, inc=1, device_id=dev(bb, xx, c), device_id_type=pl.DeviceIdType.MESH)
    if nc == 2:
        pl.semaphore_signal(barrier, inc=1, device_id=dev(b, x, other), device_id_type=pl.DeviceIdType.MESH)
    pl.semaphore_wait(barrier, len(peers) + (nc == 2))

    def remote(src, dst, s_sem, r_sem, where):
        return pltpu.make_async_remote_copy(
            src_ref=src, dst_ref=dst, send_sem=s_sem, recv_sem=r_sem,
            device_id=where, device_id_type=pl.DeviceIdType.MESH,
        )

    for cp in loads[:4]:
        cp.wait()
    slice_sends, root_sends = [], []
    for sx in range(1, nx):
        bb, xx = shifted(0, sx)
        blk = sliceb.at[x, c]
        slice_sends.append(remote(blk, blk, gs_slice.at[sx], gr_slice.at[sx], dev(b, xx, c)))
    for i, (sb, sx) in enumerate(peers):
        bb, xx = shifted(sb, sx)
        blk = rootb.at[b, x, c]
        root_sends.append(remote(blk, blk, gs_root.at[i], gr_root.at[i], dev(bb, xx, c)))
    for cp in root_sends + slice_sends:
        cp.start()

    for cp in loads[4:]:
        cp.wait()
    live = lax.broadcasted_iota(jnp.int32, (T, D), 0) < len_ref[0]
    for h in range(H):
        cols = slice(h * D, (h + 1) * D)
        rows = slice(h * T, (h + 1) * T)
        q1, q2, q3 = split3(q_ref[:, cols])
        qs[0, rows], qs[1, rows], qs[2, rows] = q1, q2, q3
        c1, c2 = split2(jnp.where(live, do_ref[:, cols], 0.0))
        cs[0, rows], cs[1, rows] = c1, c2

    def stage(first, keys, values):
        count = keys.shape[0]
        span = slice(first, first + count)
        k1, k2, k3 = split3(keys)
        ks[span, :] = side(k1, k2, k3)
        v1, v2 = split2(values)
        vs[span, :] = side(v1, v2)
        ka, kb = split2(keys.T)
        kt[:D, span] = ka
        kt[D:, span] = kb
        va, vb = split2(values.T)
        vt[:D, span] = va
        vt[D:, span] = vb

    def score(first, count, seen):
        step = min(count, 256)

        def body(p, carry):
            rows = pl.ds(pl.multiple_of(p * pair, pair), pair)
            q1, q2, q3 = qs[0, rows, :], qs[1, rows, :], qs[2, rows, :]
            c1, c2 = cs[0, rows, :], cs[1, rows, :]
            qa, qb, qc = side(q1, q1), side(q2, q2), side(q3, q1)
            ca, cb = side(c1, c1), side(c2, c2)
            for lo in range(0, count, step):
                span = slice(first + lo, first + lo + step)
                k12 = ks[span, : 2 * D]
                k13 = side(ks[span, :D], ks[span, 2 * D :])
                s = mmt(k12, qa) + (mmt(k12, qb) + mmt(k13, qc))
                sc[span, rows] = jnp.where(seen(lo, step), s * scale, hidden)
                v12 = vs[span, :]
                dp[span, rows] = mmt(v12, ca) + mmt(v12, cb)
            return carry

        lax.fori_loop(0, n_pair, body, 0)

    def index_of(lo, step):
        return lo + lax.broadcasted_iota(jnp.int32, (step, pair), 0)

    def slot_of(step):
        return lax.broadcasted_iota(jnp.int32, (step, pair), 1) % T

    stage(n_root + n_slice, leaf_ref[0], leaf_ref[1])
    score(n_root + n_slice, T, lambda lo, step: index_of(lo, step) <= slot_of(step))

    core_sends = []
    for sx in range(1, nx):
        blk = sliceb.at[lax.rem(x + nx - sx, nx), c]
        remote(blk, blk, gs_slice.at[sx], gr_slice.at[sx], dev(b, x, c)).wait_recv()
    if nc == 2:
        cp = remote(sliceb.at[:, c], sliceb.at[:, c], cs_sem.at[0], cr_sem.at[0], dev(b, x, other))
        cp.start()
        core_sends.append(cp)
    for i, (sb, sx) in enumerate(peers):
        blk = rootb.at[lax.rem(b + nb - sb, nb), lax.rem(x + nx - sx, nx), c]
        remote(blk, blk, gs_root.at[i], gr_root.at[i], dev(b, x, c)).wait_recv()
    if nc == 2:
        cp = remote(rootb.at[:, :, c], rootb.at[:, :, c], cs_sem.at[1], cr_sem.at[1], dev(b, x, other))
        cp.start()
        core_sends.append(cp)
        remote(sliceb.at[:, other], sliceb.at[:, other], cs_sem.at[0], cr_sem.at[0], dev(b, x, other)).wait_recv()
    stage(
        n_root,
        sliceb[:, :, 0].reshape(n_slice, D),
        sliceb[:, :, 1].reshape(n_slice, D),
    )
    score(n_root, n_slice, lambda lo, step: index_of(lo, step) <= par_ref[0])
    if nc == 2:
        remote(rootb.at[:, :, other], rootb.at[:, :, other], cs_sem.at[1], cr_sem.at[1], dev(b, x, other)).wait_recv()
    stage(
        0,
        rootb[:, :, :, 0].reshape(n_root, D),
        rootb[:, :, :, 1].reshape(n_root, D),
    )
    score(0, n_root, lambda lo, step: index_of(lo, step) < cut_ref[0])

    chunk = 128

    def soften(p, carry):
        rows = pl.ds(pl.multiple_of(p * pair, pair), pair)
        spans = [slice(lo, lo + chunk) for lo in range(0, n_keys, chunk)]
        top = None
        for span in spans:
            m = jnp.max(sc[span, rows], axis=0, keepdims=True)
            top = m if top is None else jnp.maximum(top, m)
        total = jnp.zeros((1, pair), f32)
        dot = jnp.zeros((1, pair), f32)
        for span in spans:
            e = jnp.exp(sc[span, rows] - top)
            sc[span, rows] = e
            total = total + jnp.sum(e, axis=0, keepdims=True)
            dot = dot + jnp.sum(e * dp[span, rows], axis=0, keepdims=True)
        inverse = 1.0 / total
        dot = dot * inverse
        for span in spans:
            w = sc[span, rows] * inverse
            sc[span, rows] = w
            dp[span, rows] = w * (dp[span, rows] - dot) * scale
        return carry

    lax.fori_loop(0, n_pair, soften, 0)

    def key_gradients(first, step):
        span = pl.ds(first, step)
        s1, s2 = split2(dp[span, :])
        q12 = side(qs[0], qs[1])
        a = mm(s1, q12) + mm(s2, q12)
        w1, w2 = split2(sc[span, :])
        c12 = side(cs[0], cs[1])
        v = mm(w1, c12) + mm(w2, c12)
        return side(a[:, :D] + a[:, D:], v[:, :D] + v[:, D:])

    def gradient_block(i, carry):
        at = pl.multiple_of(i * chunk, chunk)
        dkv[pl.ds(at, chunk), :] = key_gradients(at, chunk)
        return carry

    root_g = dkv.at[:n_root].reshape(nb, nx, nc, r_rows, 2 * D)
    slice_g = dkv.at[n_root : n_root + n_slice].reshape(nx, nc, b_rows, 2 * D)
    lax.fori_loop(0, n_root // chunk, gradient_block, 0)
    ex = []
    if nc == 2:
        cp = remote(root_g.at[:, :, other], rc_root, es_sem.at[0], er_sem.at[0], dev(b, x, other))
        cp.start()
        ex.append(cp)
    lax.fori_loop(n_root // chunk, (n_root + n_slice) // chunk, gradient_block, 0)
    if nc == 2:
        cp = remote(slice_g.at[:, other], rc_slice, es_sem.at[1], er_sem.at[1], dev(b, x, other))
        cp.start()
        ex.append(cp)
        ex[0].wait_recv()
    mine = root_g[:, :, c]
    sn_root[...] = mine + rc_root[...] if nc == 2 else mine
    fin_root = []
    for i, (sb, sx) in enumerate(peers):
        bb, xx = shifted(sb, sx)
        fin_root.append(remote(sn_root.at[bb, xx], rv_root.at[i], ss_root.at[i], sr_root.at[i], dev(bb, xx, c)))
        fin_root[-1].start()
    if nc == 2:
        ex[1].wait_recv()
    mine = slice_g[:, c]
    sn_slice[...] = mine + rc_slice[...] if nc == 2 else mine
    fin_slice = []
    for sx in range(1, nx):
        bb, xx = shifted(0, sx)
        fin_slice.append(
            remote(sn_slice.at[xx], rv_slice.at[sx - 1], ss_slice.at[sx], sr_slice.at[sx], dev(b, xx, c))
        )
        fin_slice[-1].start()

    def outputs(p, carry):
        rows = pl.ds(pl.multiple_of(p * pair, pair), pair)
        w1, w2 = split2(sc[:, rows])
        m = mm(vt[...], w1) + mm(vt[...], w2)
        m = m[:D] + m[D:]
        s1, s2 = split2(dp[:, rows])
        n = mm(kt[...], s1) + mm(kt[...], s2)
        n = n[:D] + n[D:]
        for k in range(per):
            cols = pl.ds(pl.multiple_of(p * (per * D) + k * D, D), D)
            part = slice(k * T, (k + 1) * T)
            att_ref[:, cols] = jnp.where(live, m[:, part].T, 0.0)
            dqv_ref[:, cols] = n[:, part].T
        return carry

    lax.fori_loop(0, n_pair, outputs, 0)
    dleaf_ref[...] = key_gradients(n_root + n_slice, T)

    for cp in fin_slice:
        cp.wait_recv()
    total = sn_slice[x]
    for i in range(nx - 1):
        total = total + rv_slice[i]
    dslice_ref[...] = total
    for cp in fin_root:
        cp.wait_recv()
    total = sn_root[b, x]
    for i in range(len(peers)):
        total = total + rv_root[i]
    droot_ref[...] = total
    for cp in root_sends + slice_sends + core_sends + ex + fin_root + fin_slice:
        cp.wait_send()


def deliver(*refs):
    sources, targets, sem = refs[:5], refs[5:10], refs[10]
    copies = [pltpu.make_async_copy(s, t, sem.at[i]) for i, (s, t) in enumerate(zip(sources, targets))]
    for cp in copies:
        cp.start()
    for cp in copies:
        cp.wait()


def shards(mesh, *args):
    queries, leaf_keys, _, root_keys, _, branch_keys = args[:6]
    T, width = queries.shape
    D = leaf_keys.shape[1]
    H = width // D
    r_rows, b_rows = root_keys.shape[0], branch_keys.shape[0]
    nb, nl = mesh.shape["branch"], mesh.shape["leaf"]
    nc = 2 if nl % 2 == 0 else 1
    nx = nl // nc
    R = T * H
    n_root, n_slice = nb * nl * r_rows, nl * b_rows
    n_keys = n_root + n_slice + T
    any_space = pl.BlockSpec(memory_space=pl.ANY)
    hbm = pl.BlockSpec(memory_space=pltpu.HBM)
    vmem = pl.BlockSpec(memory_space=pltpu.VMEM)
    V = pltpu.VMEM
    S = pltpu.SMEM
    dma = pltpu.SemaphoreType.DMA
    np_ = max(nb * nx - 1, 1)
    scratch = [
        V((T, width), f32), V((T, width), f32), V((2, T, D), f32),
        V((nb, nx, nc, 2, r_rows, D), f32), V((nx, nc, 2, b_rows, D), f32),
        V((3, R, D), bf16), V((2, R, D), bf16),
        V((n_keys, 3 * D), bf16), V((n_keys, 2 * D), bf16),
        V((2 * D, n_keys), bf16), V((2 * D, n_keys), bf16),
        V((n_keys, R), f32), V((n_keys, R), f32), V((n_root + n_slice, 2 * D), f32),
        S((1,), jnp.int32), S((1,), jnp.int32), S((1,), jnp.int32),
        V((nb, nx, r_rows, 2 * D), f32), V((nx, b_rows, 2 * D), f32),
        V((nb, nx, r_rows, 2 * D), f32), V((nx, b_rows, 2 * D), f32),
        V((np_, r_rows, 2 * D), f32), V((max(nx - 1, 1), b_rows, 2 * D), f32),
        dma((11,)), dma((np_,)), dma((np_,)), dma((nx,)), dma((nx,)), dma((2,)), dma((2,)),
        dma((np_,)), dma((np_,)), dma((nx,)), dma((nx,)), dma((2,)), dma((2,)),
    ]
    shape = lambda *s: V(s, f32)
    sizes = ((T, width), (T, width), (r_rows, 2 * D), (b_rows, 2 * D), (T, 2 * D))
    held = pl.pallas_call(
        functools.partial(kernel, nb, nx, nc, (T, H, D, r_rows, b_rows)),
        out_shape=tuple(shape(*size) for size in sizes),
        in_specs=[any_space] * 8 + [hbm] * 3,
        out_specs=(vmem,) * 5,
        scratch_shapes=scratch,
        compiler_params=pltpu.CompilerParams(
            collective_id=0, has_side_effects=True, vmem_limit_bytes=60 * 1024 * 1024
        ),
        name="tree",
    )(*args)
    return pl.pallas_call(
        deliver,
        out_shape=tuple(jax.ShapeDtypeStruct(size, f32) for size in sizes),
        in_specs=[vmem] * 5,
        out_specs=(any_space,) * 5,
        scratch_shapes=[dma((5,))],
        compiler_params=pltpu.CompilerParams(vmem_limit_bytes=1024 * 1024),
        name="deliver",
    )(*held)


def solution(mesh):
    rows = P(("groups", "branch", "leaf"), None)
    flat = P(("groups", "branch", "leaf"))
    return jax.shard_map(
        functools.partial(shards, mesh),
        mesh=mesh,
        in_specs=(rows,) * 8 + (flat, flat, P(("groups", "branch"))),
        out_specs=(rows,) * 5,
        check_vma=False,
    )
```

```python
import functools
import math

import jax
import jax.numpy as jnp
from jax import lax
from jax.experimental import pallas as pl
from jax.experimental.pallas import tpu as pltpu
from jax.sharding import PartitionSpec as P

f32 = jnp.float32
bf16 = jnp.bfloat16
hidden = -1e30


def split2(x):
    high = x.astype(bf16)
    return high, (x - high.astype(f32)).astype(bf16)


def split3(x):
    high = x.astype(bf16)
    rest = x - high.astype(f32)
    middle = rest.astype(bf16)
    return high, middle, (rest - middle.astype(f32)).astype(bf16)


def mm(a, b):
    return lax.dot_general(a, b, (((1,), (0,)), ((), ())), preferred_element_type=f32)


def mmt(a, b):
    return lax.dot_general(a, b, (((1,), (1,)), ((), ())), preferred_element_type=f32)


def side(*parts):
    return jnp.concatenate(parts, axis=1)


def kernel(
    nb, nx, nc, dims,
    q_hbm, lk_hbm, lv_hbm, rk_hbm, rv_hbm, bk_hbm, bv_hbm, do_hbm, len_hbm, par_hbm, cut_hbm,
    att_ref, dqv_ref, droot_ref, dslice_ref, dleaf_ref,
    q_ref, do_ref, leaf_ref, rootb, sliceb,
    qs, cs, ks, vs, kt, vt, sc, dp, dkv,
    len_ref, par_ref, cut_ref,
    rc_root, rc_slice, sn_root, sn_slice, rv_root, rv_slice,
    ld_sem, gs_root, gr_root, gs_slice, gr_slice, cs_sem, cr_sem,
    ss_root, sr_root, ss_slice, sr_slice, es_sem, er_sem,
):
    T, H, D, r_rows, b_rows = dims
    R = T * H
    n_root = nb * nx * nc * r_rows
    n_slice = nx * nc * b_rows
    n_keys = n_root + n_slice + T
    scale = 1.0 / math.sqrt(D)
    g = lax.axis_index("groups")
    b = lax.axis_index("branch")
    leaf = lax.axis_index("leaf")
    x = leaf // nc
    c = leaf % nc
    pair = 2 * T if H % 2 == 0 else T
    per = pair // T
    n_pair = R // pair

    def dev(bb, xx, cc):
        return (g, bb, xx * nc + cc)

    def shifted(sb, sx):
        return lax.rem(b + sb, nb), lax.rem(x + sx, nx)

    peers = [(sb, sx) for sb in range(nb) for sx in range(nx) if sb or sx]
    other = lax.rem(c + 1, nc)

    loads = [
        (rk_hbm, rootb.at[b, x, c, 0]),
        (rv_hbm, rootb.at[b, x, c, 1]),
        (bk_hbm, sliceb.at[x, c, 0]),
        (bv_hbm, sliceb.at[x, c, 1]),
        (lk_hbm, leaf_ref.at[0]),
        (lv_hbm, leaf_ref.at[1]),
        (q_hbm, q_ref),
        (do_hbm, do_ref),
        (len_hbm, len_ref),
        (par_hbm, par_ref),
        (cut_hbm, cut_ref),
    ]
    loads = [pltpu.make_async_copy(s, d, ld_sem.at[i]) for i, (s, d) in enumerate(loads)]
    for cp in loads:
        cp.start()

    barrier = pltpu.get_barrier_semaphore()
    for sb, sx in peers:
        bb, xx = shifted(sb, sx)
        pl.semaphore_signal(barrier, inc=1, device_id=dev(bb, xx, c), device_id_type=pl.DeviceIdType.MESH)
    if nc == 2:
        pl.semaphore_signal(barrier, inc=1, device_id=dev(b, x, other), device_id_type=pl.DeviceIdType.MESH)
    pl.semaphore_wait(barrier, len(peers) + (nc == 2))

    def remote(src, dst, s_sem, r_sem, where):
        return pltpu.make_async_remote_copy(
            src_ref=src, dst_ref=dst, send_sem=s_sem, recv_sem=r_sem,
            device_id=where, device_id_type=pl.DeviceIdType.MESH,
        )

    for cp in loads[:4]:
        cp.wait()
    slice_sends, root_sends = [], []
    for sx in range(1, nx):
        bb, xx = shifted(0, sx)
        blk = sliceb.at[x, c]
        slice_sends.append(remote(blk, blk, gs_slice.at[sx], gr_slice.at[sx], dev(b, xx, c)))
    for i, (sb, sx) in enumerate(peers):
        bb, xx = shifted(sb, sx)
        blk = rootb.at[b, x, c]
        root_sends.append(remote(blk, blk, gs_root.at[i], gr_root.at[i], dev(bb, xx, c)))
    for cp in root_sends + slice_sends:
        cp.start()

    for cp in loads[4:]:
        cp.wait()
    live = lax.broadcasted_iota(jnp.int32, (T, D), 0) < len_ref[0]
    for h in range(H):
        cols = slice(h * D, (h + 1) * D)
        rows = slice(h * T, (h + 1) * T)
        q1, q2, q3 = split3(q_ref[:, cols])
        qs[0, rows], qs[1, rows], qs[2, rows] = q1, q2, q3
        c1, c2 = split2(jnp.where(live, do_ref[:, cols], 0.0))
        cs[0, rows], cs[1, rows] = c1, c2

    def stage(first, keys, values):
        count = keys.shape[0]
        span = slice(first, first + count)
        k1, k2, k3 = split3(keys)
        ks[span, :] = side(k1, k2, k3)
        v1, v2 = split2(values)
        vs[span, :] = side(v1, v2)
        ka, kb = split2(keys.T)
        kt[:D, span] = ka
        kt[D:, span] = kb
        va, vb = split2(values.T)
        vt[:D, span] = va
        vt[D:, span] = vb

    def score(first, count, seen):
        step = min(count, 256)

        def body(p, carry):
            rows = pl.ds(pl.multiple_of(p * pair, pair), pair)
            q1, q2, q3 = qs[0, rows, :], qs[1, rows, :], qs[2, rows, :]
            c1, c2 = cs[0, rows, :], cs[1, rows, :]
            qa, qb, qc = side(q1, q1), side(q2, q2), side(q3, q1)
            ca, cb = side(c1, c1), side(c2, c2)
            for lo in range(0, count, step):
                span = slice(first + lo, first + lo + step)
                k12 = ks[span, : 2 * D]
                k13 = side(ks[span, :D], ks[span, 2 * D :])
                s = mmt(k12, qa) + (mmt(k12, qb) + mmt(k13, qc))
                sc[span, rows] = jnp.where(seen(lo, step), s * scale, hidden)
                v12 = vs[span, :]
                dp[span, rows] = mmt(v12, ca) + mmt(v12, cb)
            return carry

        lax.fori_loop(0, n_pair, body, 0)

    def index_of(lo, step):
        return lo + lax.broadcasted_iota(jnp.int32, (step, pair), 0)

    def slot_of(step):
        return lax.broadcasted_iota(jnp.int32, (step, pair), 1) % T

    stage(n_root + n_slice, leaf_ref[0], leaf_ref[1])
    score(n_root + n_slice, T, lambda lo, step: index_of(lo, step) <= slot_of(step))

    core_sends = []
    for sx in range(1, nx):
        blk = sliceb.at[lax.rem(x + nx - sx, nx), c]
        remote(blk, blk, gs_slice.at[sx], gr_slice.at[sx], dev(b, x, c)).wait_recv()
    if nc == 2:
        cp = remote(sliceb.at[:, c], sliceb.at[:, c], cs_sem.at[0], cr_sem.at[0], dev(b, x, other))
        cp.start()
        core_sends.append(cp)
    for i, (sb, sx) in enumerate(peers):
        blk = rootb.at[lax.rem(b + nb - sb, nb), lax.rem(x + nx - sx, nx), c]
        remote(blk, blk, gs_root.at[i], gr_root.at[i], dev(b, x, c)).wait_recv()
    if nc == 2:
        cp = remote(rootb.at[:, :, c], rootb.at[:, :, c], cs_sem.at[1], cr_sem.at[1], dev(b, x, other))
        cp.start()
        core_sends.append(cp)
        remote(sliceb.at[:, other], sliceb.at[:, other], cs_sem.at[0], cr_sem.at[0], dev(b, x, other)).wait_recv()
    stage(
        n_root,
        sliceb[:, :, 0].reshape(n_slice, D),
        sliceb[:, :, 1].reshape(n_slice, D),
    )
    score(n_root, n_slice, lambda lo, step: index_of(lo, step) <= par_ref[0])
    if nc == 2:
        remote(rootb.at[:, :, other], rootb.at[:, :, other], cs_sem.at[1], cr_sem.at[1], dev(b, x, other)).wait_recv()
    stage(
        0,
        rootb[:, :, :, 0].reshape(n_root, D),
        rootb[:, :, :, 1].reshape(n_root, D),
    )
    score(0, n_root, lambda lo, step: index_of(lo, step) < cut_ref[0])

    chunk = 128

    def soften(p, carry):
        rows = pl.ds(pl.multiple_of(p * pair, pair), pair)
        spans = [slice(lo, lo + chunk) for lo in range(0, n_keys, chunk)]
        top = None
        for span in spans:
            m = jnp.max(sc[span, rows], axis=0, keepdims=True)
            top = m if top is None else jnp.maximum(top, m)
        total = jnp.zeros((1, pair), f32)
        dot = jnp.zeros((1, pair), f32)
        for span in spans:
            e = jnp.exp(sc[span, rows] - top)
            sc[span, rows] = e
            total = total + jnp.sum(e, axis=0, keepdims=True)
            dot = dot + jnp.sum(e * dp[span, rows], axis=0, keepdims=True)
        inverse = 1.0 / total
        dot = dot * inverse
        for span in spans:
            w = sc[span, rows] * inverse
            sc[span, rows] = w
            dp[span, rows] = w * (dp[span, rows] - dot) * scale
        return carry

    lax.fori_loop(0, n_pair, soften, 0)

    def key_gradients(first, step):
        span = pl.ds(first, step)
        s1, s2 = split2(dp[span, :])
        q12 = side(qs[0], qs[1])
        a = mm(s1, q12) + mm(s2, q12)
        w1, w2 = split2(sc[span, :])
        c12 = side(cs[0], cs[1])
        v = mm(w1, c12) + mm(w2, c12)
        return side(a[:, :D] + a[:, D:], v[:, :D] + v[:, D:])

    block = 2 * chunk if n_root % (2 * chunk) == 0 and n_slice % (2 * chunk) == 0 else chunk

    def gradient_block(i, carry):
        at = pl.multiple_of(i * block, block)
        dkv[pl.ds(at, block), :] = key_gradients(at, block)
        return carry

    root_g = dkv.at[:n_root].reshape(nb, nx, nc, r_rows, 2 * D)
    slice_g = dkv.at[n_root : n_root + n_slice].reshape(nx, nc, b_rows, 2 * D)
    lax.fori_loop(0, n_root // block, gradient_block, 0)
    ex = []
    if nc == 2:
        cp = remote(root_g.at[:, :, other], rc_root, es_sem.at[0], er_sem.at[0], dev(b, x, other))
        cp.start()
        ex.append(cp)
    lax.fori_loop(n_root // block, (n_root + n_slice) // block, gradient_block, 0)
    if nc == 2:
        cp = remote(slice_g.at[:, other], rc_slice, es_sem.at[1], er_sem.at[1], dev(b, x, other))
        cp.start()
        ex.append(cp)
        ex[0].wait_recv()
    mine = root_g[:, :, c]
    sn_root[...] = mine + rc_root[...] if nc == 2 else mine
    fin_root = []
    for i, (sb, sx) in enumerate(peers):
        bb, xx = shifted(sb, sx)
        fin_root.append(remote(sn_root.at[bb, xx], rv_root.at[i], ss_root.at[i], sr_root.at[i], dev(bb, xx, c)))
        fin_root[-1].start()
    if nc == 2:
        ex[1].wait_recv()
    mine = slice_g[:, c]
    sn_slice[...] = mine + rc_slice[...] if nc == 2 else mine
    fin_slice = []
    for sx in range(1, nx):
        bb, xx = shifted(0, sx)
        fin_slice.append(
            remote(sn_slice.at[xx], rv_slice.at[sx - 1], ss_slice.at[sx], sr_slice.at[sx], dev(b, xx, c))
        )
        fin_slice[-1].start()

    def outputs(p, carry):
        rows = pl.ds(pl.multiple_of(p * pair, pair), pair)
        w1, w2 = split2(sc[:, rows])
        m = mm(vt[...], w1) + mm(vt[...], w2)
        m = m[:D] + m[D:]
        s1, s2 = split2(dp[:, rows])
        n = mm(kt[...], s1) + mm(kt[...], s2)
        n = n[:D] + n[D:]
        for k in range(per):
            cols = pl.ds(pl.multiple_of(p * (per * D) + k * D, D), D)
            part = slice(k * T, (k + 1) * T)
            att_ref[:, cols] = jnp.where(live, m[:, part].T, 0.0)
            dqv_ref[:, cols] = n[:, part].T
        return carry

    lax.fori_loop(0, n_pair, outputs, 0)
    dleaf_ref[...] = key_gradients(n_root + n_slice, T)

    for cp in fin_slice:
        cp.wait_recv()
    total = sn_slice[x]
    for i in range(nx - 1):
        total = total + rv_slice[i]
    dslice_ref[...] = total
    for cp in fin_root:
        cp.wait_recv()
    total = sn_root[b, x]
    for i in range(len(peers)):
        total = total + rv_root[i]
    droot_ref[...] = total
    for cp in root_sends + slice_sends + core_sends + ex + fin_root + fin_slice:
        cp.wait_send()


def deliver(*refs):
    sources, targets, sem = refs[:5], refs[5:10], refs[10]
    copies = [pltpu.make_async_copy(s, t, sem.at[i]) for i, (s, t) in enumerate(zip(sources, targets))]
    for cp in copies:
        cp.start()
    for cp in copies:
        cp.wait()


def shards(mesh, *args):
    queries, leaf_keys, _, root_keys, _, branch_keys = args[:6]
    T, width = queries.shape
    D = leaf_keys.shape[1]
    H = width // D
    r_rows, b_rows = root_keys.shape[0], branch_keys.shape[0]
    nb, nl = mesh.shape["branch"], mesh.shape["leaf"]
    nc = 2 if nl % 2 == 0 else 1
    nx = nl // nc
    R = T * H
    n_root, n_slice = nb * nl * r_rows, nl * b_rows
    n_keys = n_root + n_slice + T
    any_space = pl.BlockSpec(memory_space=pl.ANY)
    hbm = pl.BlockSpec(memory_space=pltpu.HBM)
    vmem = pl.BlockSpec(memory_space=pltpu.VMEM)
    V = pltpu.VMEM
    S = pltpu.SMEM
    dma = pltpu.SemaphoreType.DMA
    np_ = max(nb * nx - 1, 1)
    scratch = [
        V((T, width), f32), V((T, width), f32), V((2, T, D), f32),
        V((nb, nx, nc, 2, r_rows, D), f32), V((nx, nc, 2, b_rows, D), f32),
        V((3, R, D), bf16), V((2, R, D), bf16),
        V((n_keys, 3 * D), bf16), V((n_keys, 2 * D), bf16),
        V((2 * D, n_keys), bf16), V((2 * D, n_keys), bf16),
        V((n_keys, R), f32), V((n_keys, R), f32), V((n_root + n_slice, 2 * D), f32),
        S((1,), jnp.int32), S((1,), jnp.int32), S((1,), jnp.int32),
        V((nb, nx, r_rows, 2 * D), f32), V((nx, b_rows, 2 * D), f32),
        V((nb, nx, r_rows, 2 * D), f32), V((nx, b_rows, 2 * D), f32),
        V((np_, r_rows, 2 * D), f32), V((max(nx - 1, 1), b_rows, 2 * D), f32),
        dma((11,)), dma((np_,)), dma((np_,)), dma((nx,)), dma((nx,)), dma((2,)), dma((2,)),
        dma((np_,)), dma((np_,)), dma((nx,)), dma((nx,)), dma((2,)), dma((2,)),
    ]
    shape = lambda *s: V(s, f32)
    sizes = ((T, width), (T, width), (r_rows, 2 * D), (b_rows, 2 * D), (T, 2 * D))
    held = pl.pallas_call(
        functools.partial(kernel, nb, nx, nc, (T, H, D, r_rows, b_rows)),
        out_shape=tuple(shape(*size) for size in sizes),
        in_specs=[any_space] * 8 + [hbm] * 3,
        out_specs=(vmem,) * 5,
        scratch_shapes=scratch,
        compiler_params=pltpu.CompilerParams(
            collective_id=0, has_side_effects=True, vmem_limit_bytes=60 * 1024 * 1024
        ),
        name="tree",
    )(*args)
    return pl.pallas_call(
        deliver,
        out_shape=tuple(jax.ShapeDtypeStruct(size, f32) for size in sizes),
        in_specs=[vmem] * 5,
        out_specs=(any_space,) * 5,
        scratch_shapes=[dma((5,))],
        compiler_params=pltpu.CompilerParams(vmem_limit_bytes=1024 * 1024),
        name="deliver",
    )(*held)


def solution(mesh):
    rows = P(("groups", "branch", "leaf"), None)
    flat = P(("groups", "branch", "leaf"))
    return jax.shard_map(
        functools.partial(shards, mesh),
        mesh=mesh,
        in_specs=(rows,) * 8 + (flat, flat, P(("groups", "branch"))),
        out_specs=(rows,) * 5,
        check_vma=False,
    )
```
